256 devices in a mesh: depth: 64 (over z_lo, y, x, core), lane: 4 (over z_hi).
Axes of the slice: x: 4, y: 4, z: 8 (z_hi: 4, z_lo: 2; z = z_hi * 2 + z_lo), core: 2. Of those that a mesh axis runs over, the one named last changes fastest.
Arguments:
- fields_in: float32 [64, 4, 16, 1024], P('depth', None, 'lane'), may hold values from -6 to 6
- shot_data: float32 [4, 128, 2, 16, 1024], P(None, 'depth', None, 'lane'), may hold values from -0.5 to 0.5
- codes: int32 [4, 128, 16], P(None, None, 'lane'), may hold values from 0 to 15
- vel_index: int32 [256, 1024], P('depth'), may hold values from 0 to 63
- slowness_table: float32 [64], replicated, may hold values from 0.4 to 1
Outputs:
- fields_out: float32 [64, 4, 16, 1024], P('depth', None, 'lane')
- image: float32 [256, 1024], P(('depth', 'lane'))
The draws below stay inside these ranges and needn't reach their ends.
All inputs are finite; a program needn't handle non-finite values.
Results may differ from the reference program's by a relative error of at most 0.0003.
Values sent between devices are 32-bit elements; how exact they have to be, the bound alone decides.
No kernel may reach another device: no remote copies, remote signals or barrier semaphores. Data moves between devices by JAX's collectives and lax.ppermute only.
A program may use at most 64 MiB of HBM per device.

```python
import math
import jax
import jax.numpy as jnp
from jax import lax

NX = 1024
STEPS = 4
TICKS = 4
LEVELS = 64
CODES = 16
SECTIONS = 64
NZ = 256
NF = 16
SHOTS = 128


def touch_ends(result, own_key, least, largest):
    longest = result.shape.index(max(result.shape))
    spots = []
    for shift in (0, 1):
        where = [jax.random.randint(jax.random.fold_in(own_key, axis), (), 0, length) for axis, length in enumerate(result.shape)]
        where[longest] = (where[longest] + shift) % result.shape[longest]
        spots.append(tuple(where))
    return result.at[spots[0]].set(least).at[spots[1]].set(largest)


def block_scale(stream_key, extent, split, smallest, largest):
    factor_of = 1.0
    for dim, shards_of in split:
        heights = jax.random.uniform(jax.random.fold_in(jax.random.fold_in(stream_key, 6), dim), (shards_of,), jnp.float32, smallest / len(split), largest / len(split))
        factor_of = factor_of * jnp.repeat(jnp.exp(heights), extent[dim] // shards_of).reshape((-1,) + (1,) * (len(extent) - 1 - dim))
    return factor_of


def scatter_about(key, shape, spread, limit, pieces=(), kind=jnp.bfloat16):
    result = jax.random.normal(key, shape, jnp.float32) * spread
    if len(pieces) > 0:
        result = block_scale(key, shape, pieces, -0.22, 0.18) * result
    return jnp.clip(result, min=-limit, max=limit).astype(kind)


def setup_inputs(seed: int = 0) -> dict:
    arg_keys = jax.random.split(jax.random.key(seed), 6)
    return {
        "fields_in": scatter_about(arg_keys[0], (SECTIONS, 4, NF, NX), 1.0, 6.0, ((0, 64), (2, 4)), jnp.float32),
        "shot_data": scatter_about(arg_keys[1], (TICKS, SHOTS, 2, NF, NX), SHOTS ** -0.5, 0.5, ((1, 64), (3, 4)), jnp.float32),
        "codes": touch_ends(jax.random.randint(arg_keys[2], (TICKS, SHOTS, NF), 0, CODES), jax.random.fold_in(arg_keys[2], 1), 0, CODES - 1).astype(jnp.int32),
        "vel_index": touch_ends(jax.random.randint(arg_keys[3], (NZ, NX), 0, LEVELS), jax.random.fold_in(arg_keys[3], 1), 0, LEVELS - 1).astype(jnp.int32),
        "slowness_table": jnp.clip(jnp.exp(jax.random.uniform(arg_keys[4], (LEVELS,), jnp.float32, math.log(0.4), math.log(1.0))), 0.4, 1.0),
    }


OMEGA_LO = 0.25
OMEGA_STEP = 0.07
DEPTH_STEP = 1.0
TWO_PI = 6.283185307179586

def wavenumbers(points):
    index = jnp.arange(points, dtype=jnp.int32)
    signed = jnp.where(index < points // 2, index, index - points)
    return signed.astype(jnp.float32) * (TWO_PI / points)

def reference(fields_in, shot_data, codes, vel_index, slowness_table):
    source = fields_in[:, 0] + 1j * fields_in[:, 1]
    receiver = fields_in[:, 2] + 1j * fields_in[:, 3]
    omegas = OMEGA_LO + OMEGA_STEP * jnp.arange(NF, dtype=jnp.int32).astype(jnp.float32)
    kx_sq = wavenumbers(NX) ** 2
    slowness = jnp.take(slowness_table, vel_index, axis=0).reshape(SECTIONS, STEPS, NX)
    angles = codes.astype(jnp.float32) * (TWO_PI / CODES)
    encode = jnp.cos(angles) + 1j * jnp.sin(angles)
    records = shot_data[:, :, 0] + 1j * shot_data[:, :, 1]
    rec_in = lax.optimization_barrier(jnp.sum(encode[:, :, :, None] * records, axis=1))
    spacing = NX // SHOTS
    marker = (jnp.arange(spacing, dtype=jnp.int32) == 0).astype(jnp.float32)
    src_in = (jnp.transpose(encode, (0, 2, 1))[:, :, :, None] * marker).reshape(TICKS, NF, NX)
    image = jnp.zeros((SECTIONS, STEPS, NX), jnp.float32)
    for tick_index in range(TICKS):
        for step_index in range(STEPS):
            slow_row = slowness[:, step_index]
            ref_slow = lax.optimization_barrier(jnp.mean(slow_row, axis=-1, keepdims=True))
            kz_sq = (omegas[None, :, None] * ref_slow[:, None, :]) ** 2 - kx_sq[None, None, :]
            phases = jnp.sqrt(jnp.maximum(kz_sq, 0.0)) * DEPTH_STEP
            damping = jnp.exp(-jnp.sqrt(jnp.maximum(-kz_sq, 0.0)) * DEPTH_STEP)
            lens_angle = omegas[None, :, None] * (slow_row - ref_slow)[:, None, :] * DEPTH_STEP
            turn = jnp.cos(phases) + 1j * jnp.sin(phases)
            lens_turn = jnp.cos(lens_angle) + 1j * jnp.sin(lens_angle)
            source = jnp.fft.ifft(jnp.fft.fft(source, axis=-1) * damping * turn, axis=-1) * lens_turn
            receiver = jnp.fft.ifft(jnp.fft.fft(receiver, axis=-1) * damping * jnp.conj(turn), axis=-1) * jnp.conj(lens_turn)
            contrib = lax.optimization_barrier(jnp.sum(jnp.real(source) * jnp.real(receiver) + jnp.imag(source) * jnp.imag(receiver), axis=1)) / NF
            image = image.at[:, step_index].add(contrib)
        source = jnp.concatenate([src_in[tick_index][None], source[:-1]], axis=0)
        receiver = jnp.concatenate([rec_in[tick_index][None], receiver[:-1]], axis=0)
    fields_out = jnp.stack([jnp.real(source), jnp.imag(source), jnp.real(receiver), jnp.imag(receiver)], axis=1)
    return (fields_out, image.reshape(NZ, NX))
```

```python
import functools
import math

import jax
import jax.numpy as jnp
import numpy as np
from jax import lax
from jax.experimental import pallas as pl
from jax.experimental.pallas import tpu as pltpu
from jax.sharding import PartitionSpec as P


CODES = 16
OMEGA_LO = 0.25
OMEGA_STEP = 0.07
TWO_PI = 6.283185307179586
LANES = 128
OUTER = 8
F32 = jnp.float32
BF16 = jnp.bfloat16
VMEM = pl.BlockSpec(memory_space=pltpu.VMEM)
SMEM = pl.BlockSpec(memory_space=pltpu.SMEM)


def dft_tables():
    j = np.arange(LANES)
    angle = 2.0 * np.pi * (np.outer(j, j) % LANES) / LANES
    c, s = np.cos(angle), np.sin(angle)
    full = np.block([[c, -s], [s, c]])
    high = np.asarray(full, dtype=BF16)
    low = np.asarray(full - high.astype(np.float64), dtype=BF16)
    k1 = np.repeat(np.arange(OUTER), 8)
    twist = 2.0 * np.pi * np.outer(k1, j) / (OUTER * LANES)
    turn = np.stack([np.cos(twist), np.sin(twist)]).astype(np.float32)
    return high, low, turn


def poly(coefs, x):
    out = jnp.full_like(x, coefs[-1])
    for c in reversed(coefs[:-1]):
        out = out * x + c
    return out


COS = [(-1.0) ** n / math.factorial(2 * n) for n in range(8)]
SIN = [(-1.0) ** n / math.factorial(2 * n + 1) for n in range(8)]


def cos_sin(x):
    sq = x * x
    return poly(COS, sq), x * poly(SIN, sq)


def code_turn(code):
    quarter = (code + 2) >> 2
    rest = (code - 4 * quarter).astype(F32) * (TWO_PI / CODES)
    c, s = cos_sin(rest)
    odd = (quarter & 1) == 1
    a = jnp.where(odd, -s, c)
    b = jnp.where(odd, c, s)
    flip = (quarter & 2) == 2
    return jnp.where(flip, -a, a), jnp.where(flip, -b, b)


def fourth(a, b, c, d, sign):
    s0 = (a[0] + c[0], a[1] + c[1])
    s1 = (a[0] - c[0], a[1] - c[1])
    s2 = (b[0] + d[0], b[1] + d[1])
    s3 = (b[0] - d[0], b[1] - d[1])
    plus = (s1[0] - s3[1], s1[1] + s3[0])
    minus = (s1[0] + s3[1], s1[1] - s3[0])
    x0 = (s0[0] + s2[0], s0[1] + s2[1])
    x2 = (s0[0] - s2[0], s0[1] - s2[1])
    return (x0, minus, x2, plus) if sign > 0 else (x0, plus, x2, minus)


def eighth(x, sign):
    even = fourth(x[0], x[2], x[4], x[6], sign)
    odd = fourth(x[1], x[3], x[5], x[7], sign)
    h = math.sqrt(0.5)
    o1, o2, o3 = odd[1], odd[2], odd[3]
    if sign > 0:
        w1 = ((o1[0] + o1[1]) * h, (o1[1] - o1[0]) * h)
        w2 = (o2[1], -o2[0])
        w3 = ((o3[1] - o3[0]) * h, -(o3[0] + o3[1]) * h)
    else:
        w1 = ((o1[0] - o1[1]) * h, (o1[1] + o1[0]) * h)
        w2 = (-o2[1], o2[0])
        w3 = (-(o3[0] + o3[1]) * h, (o3[0] - o3[1]) * h)
    w = (odd[0], w1, w2, w3)
    low = [(e[0] + v[0], e[1] + v[1]) for e, v in zip(even, w)]
    high = [(e[0] - v[0], e[1] - v[1]) for e, v in zip(even, w)]
    return low + high


def times(x, y):
    return (x[0] * y[0] - x[1] * y[1], x[0] * y[1] + x[1] * y[0])


def times_conj(x, y):
    return (x[0] * y[0] + x[1] * y[1], x[1] * y[0] - x[0] * y[1])


def mix(first, second, high_ref, low_ref):
    left = jnp.concatenate(first, axis=0)
    right = jnp.concatenate(second, axis=0)
    value = jnp.concatenate([left, right], axis=1)
    high = value.astype(BF16)
    low = (value - high.astype(F32)).astype(BF16)
    rows = value.shape[0]
    main = jnp.dot(
        jnp.concatenate([high, low], axis=0), high_ref[...], preferred_element_type=F32
    )
    rest = jnp.dot(high, low_ref[...], preferred_element_type=F32)
    out = main[:rows] + main[rows:] + rest
    split = lambda part: [part[8 * k : 8 * k + 8] for k in range(OUTER)]
    return split(out[:, :LANES]), split(out[:, LANES:])


def run_steps(tiles, lane, slow_ref, high_ref, low_ref, turn_ref, image_ref, freq_total):
    points = OUTER * LANES
    steps = slow_ref.shape[0]
    row = lax.broadcasted_iota(jnp.int32, (8, LANES), 0)
    column = lax.broadcasted_iota(jnp.int32, (8, LANES), 1)
    freq = lane * 4 + (row & 3)
    omega = OMEGA_LO + OMEGA_STEP * freq.astype(F32)
    turn = [
        (turn_ref[0, 8 * k : 8 * k + 8, :], turn_ref[1, 8 * k : 8 * k + 8, :])
        for k in range(OUTER)
    ]
    kx_sq = []
    for k in range(OUTER):
        index = k + OUTER * column
        signed = jnp.where(index < points // 2, index, index - points)
        kx_sq.append((signed.astype(F32) * (TWO_PI / points)) ** 2)
    slow = slow_ref[...]
    mean = jnp.sum(slow, axis=1, keepdims=True) * (1.0 / points)
    for step in range(steps):
        ref = jnp.broadcast_to(mean[step : step + 1], (8, LANES))
        bound = (omega * ref) ** 2
        spec = eighth(tiles, 1)
        spec = [spec[0]] + [times_conj(spec[k], turn[k]) for k in range(1, OUTER)]
        re, im = mix([v[0] for v in spec], [v[1] for v in spec], high_ref, low_ref)
        moved = []
        for k in range(OUTER):
            kz_sq = bound - kx_sq[k]
            root = jnp.sqrt(jnp.abs(kz_sq))
            cos, sin = cos_sin(root)
            travels = kz_sq > 0.0
            scale = 1.0 / points
            prop = (
                jnp.where(travels, cos, jnp.exp(-root)) * scale,
                jnp.where(travels, sin, 0.0) * scale,
            )
            moved.append(times((re[k], im[k]), prop))
        im, re = mix([v[1] for v in moved], [v[0] for v in moved], high_ref, low_ref)
        back = [(re[0], im[0])] + [times((re[k], im[k]), turn[k]) for k in range(1, OUTER)]
        field = eighth(back, -1)
        tiles = []
        for a in range(OUTER):
            part = jnp.broadcast_to(
                slow[step : step + 1, LANES * a : LANES * (a + 1)], (8, LANES)
            )
            lens = cos_sin(omega * (part - ref))
            tiles.append(times(field[a], lens))
        for a in range(OUTER):
            re, im = tiles[a]
            both = re * pltpu.roll(re, 4, 0) - im * pltpu.roll(im, 4, 0)
            total = jnp.sum(both, axis=0, keepdims=True) * (0.5 / freq_total)
            image_ref[step : step + 1, LANES * a : LANES * (a + 1)] = total
    return tiles


def cut(a):
    return slice(LANES * a, LANES * (a + 1))


def natural_tiles(s_re, s_im, r_re, r_im):
    return [
        (
            jnp.concatenate([s_re[:, cut(a)], r_re[:, cut(a)]], axis=0),
            jnp.concatenate([s_im[:, cut(a)], -r_im[:, cut(a)]], axis=0),
        )
        for a in range(OUTER)
    ]


def state_tiles(state_ref):
    return [
        (state_ref[0, 8 * a : 8 * a + 8, :], state_ref[1, 8 * a : 8 * a + 8, :])
        for a in range(OUTER)
    ]


def put_state(state_ref, tiles):
    for a in range(OUTER):
        state_ref[0, 8 * a : 8 * a + 8, :] = tiles[a][0]
        state_ref[1, 8 * a : 8 * a + 8, :] = tiles[a][1]


def start_kernel(place_ref, table_ref, codes_ref, index_ref, shots_ref, part_ref, slow_ref):
    place = place_ref[0]
    ticks, here = shots_ref.shape[0], shots_ref.shape[1]
    index = index_ref[...]
    slow = jnp.zeros(index.shape, F32)
    for level in range(table_ref.shape[0]):
        slow = jnp.where(index == level, table_ref[level], slow)
    slow_ref[...] = slow
    codes = codes_ref[...]
    column = lax.broadcasted_iota(jnp.int32, codes.shape, 1)
    turns = []
    for j in range(here):
        own = jnp.sum(
            jnp.where(column == place * here + j, codes, 0).astype(F32), axis=1, keepdims=True
        )
        turns.append(code_turn(own.astype(jnp.int32)))
    for t in range(ticks):
        re = im = 0.0
        for j in range(here):
            c = turns[j][0][4 * t : 4 * t + 4]
            s = turns[j][1][4 * t : 4 * t + 4]
            d_re, d_im = shots_ref[t, j, 0], shots_ref[t, j, 1]
            re = re + (c * d_re - s * d_im)
            im = im + (c * d_im + s * d_re)
        part_ref[t, 0] = re
        part_ref[t, 1] = im


def first_kernel(
    freq_total, place_ref, field_ref, slow_ref, codes_ref, high_ref, low_ref, turn_ref,
    state_ref, image_ref, source_ref,
):
    tiles = natural_tiles(field_ref[0], field_ref[1], field_ref[2], field_ref[3])
    tiles = run_steps(
        tiles, place_ref[1], slow_ref, high_ref, low_ref, turn_ref, image_ref, freq_total
    )
    put_state(state_ref, tiles)
    codes = codes_ref[...]
    shots = codes.shape[1]
    points = OUTER * LANES
    spacing = points // shots
    shot = lax.broadcasted_iota(jnp.int32, (shots, points), 0)
    cell = lax.broadcasted_iota(jnp.int32, (shots, points), 1)
    spread = jnp.where(cell == shot * spacing, 1.0, 0.0).astype(BF16)
    wide = jnp.dot(codes.astype(F32).astype(BF16), spread, preferred_element_type=F32)
    c, s = code_turn(wide.astype(jnp.int32))
    at_shot = lax.broadcasted_iota(jnp.int32, wide.shape, 1) % spacing == 0
    c = jnp.where(at_shot, c, 0.0)
    s = jnp.where(at_shot, s, 0.0)
    for t in range(codes.shape[0] // 4):
        source_ref[t, 0] = c[4 * t : 4 * t + 4]
        source_ref[t, 1] = s[4 * t : 4 * t + 4]


def injected(here, source_ref, record_ref, tick, state_ref, held_ref):
    @pl.when(here)
    def _():
        put_state(
            held_ref,
            natural_tiles(source_ref[tick, 0], source_ref[tick, 1], record_ref[0], record_ref[1]),
        )

    @pl.when(jnp.logical_not(here))
    def _():
        held_ref[...] = state_ref[...]


def middle_kernel(
    freq_total, tick, holder, place_ref, state_in_ref, record_ref, source_ref, slow_ref,
    high_ref, low_ref, turn_ref, state_ref, image_ref, held_ref,
):
    injected(place_ref[0] == holder, source_ref, record_ref, tick, state_in_ref, held_ref)
    tiles = run_steps(
        state_tiles(held_ref), place_ref[1], slow_ref, high_ref, low_ref, turn_ref, image_ref,
        freq_total,
    )
    put_state(state_ref, tiles)


def last_kernel(
    freq_total, tick, holder, final, place_ref, state_in_ref, record_ref, source_ref, slow_ref,
    high_ref, low_ref, turn_ref, image_a_ref, image_b_ref, image_c_ref, field_ref, image_ref,
    held_ref,
):
    injected(place_ref[0] == holder, source_ref, record_ref, tick, state_in_ref, held_ref)
    tiles = run_steps(
        state_tiles(held_ref), place_ref[1], slow_ref, high_ref, low_ref, turn_ref, image_ref,
        freq_total,
    )
    image_ref[...] += image_a_ref[...] + image_b_ref[...] + image_c_ref[...]
    for a in range(OUTER):
        re, im = tiles[a]
        field_ref[0, :, cut(a)] = re[:4]
        field_ref[1, :, cut(a)] = im[:4]
        field_ref[2, :, cut(a)] = re[4:]
        field_ref[3, :, cut(a)] = -im[4:]

    @pl.when(place_ref[0] == final)
    def _():
        field_ref[0] = source_ref[tick + 1, 0]
        field_ref[1] = source_ref[tick + 1, 1]
        field_ref[2] = record_ref[0]
        field_ref[3] = record_ref[1]


def per_device(sections, lanes, fields_in, shot_data, codes, vel_index, slowness_table):
    depth_pos = lax.axis_index("depth")
    lane_pos = lax.axis_index("lane")
    ticks, _, _, rows, points = shot_data.shape
    steps = vel_index.shape[0]
    freq_total = rows * lanes
    high, low, turn = dft_tables()
    place = jnp.stack([depth_pos, lane_pos]).astype(jnp.int32)
    turned = jnp.transpose(codes, (0, 2, 1)).reshape(ticks * rows, codes.shape[1])
    shape = lambda *s: jax.ShapeDtypeStruct(s, F32)
    cost = pl.CostEstimate(flops=200_000_000, bytes_accessed=1_000_000, transcendentals=0)
    state_shape = shape(2, OUTER * 8, LANES)
    image_shape = shape(steps, points)
    held = [pltpu.VMEM((2, OUTER * 8, LANES), F32)]

    partial_rec, slow = pl.pallas_call(
        start_kernel,
        out_shape=(shape(ticks, 2, rows, points), image_shape),
        in_specs=[SMEM, SMEM, VMEM, VMEM, VMEM],
        out_specs=(VMEM, VMEM),
        name="start",
    )(place, slowness_table, turned, vel_index, shot_data)

    def move(array, by, name):
        pairs = [(i, (i + by) % sections) for i in range(sections)]
        with jax.named_scope(name):
            return lax.ppermute(array, "depth", pairs)

    slow_back_1 = move(slow, 1, "slow1")
    slow_back_2 = move(slow, 2, "slow2")

    member = depth_pos % 4
    tick_of = jnp.array([2, 1, 0, 3], jnp.int32)
    pick = lambda m: lax.dynamic_index_in_dim(partial_rec, tick_of[m % 4], 0, keepdims=False)
    gathered = pick(member)
    arrived = []
    for j in (1, 2, 3):
        pairs = [(i, i - i % 4 + (i + j) % 4) for i in range(sections)]
        with jax.named_scope(f"gather{j}"):
            arrived.append(lax.ppermute(pick(member + j), "depth", pairs))
    gathered = gathered + arrived[0] + (arrived[1] + arrived[2])
    groups = sections // 4
    for stride in (1, 4):
        arrived = []
        for j in (1, 2, 3):
            pairs = []
            for m in range(4):
                for g in range(groups):
                    digit = (g // stride) % 4
                    want, to = (j, 0) if m < 3 else (3 - j, 3)
                    if digit == want:
                        goal = g + (to - digit) * stride
                        pairs.append((4 * g + m, 4 * goal + m))
            with jax.named_scope(f"reduce{stride}_{j}"):
                arrived.append(lax.ppermute(gathered, "depth", pairs))
        gathered = gathered + arrived[0] + (arrived[1] + arrived[2])

    state, image_0, source = pl.pallas_call(
        functools.partial(first_kernel, freq_total),
        out_shape=(state_shape, image_shape, shape(ticks, 2, rows, points)),
        in_specs=[SMEM] + [VMEM] * 6,
        out_specs=(VMEM, VMEM, VMEM),
        cost_estimate=cost,
        name="tick0",
    )(place, fields_in[0], slow, turned, high, low, turn)
    state = move(state, 3, "state")

    images = []
    for tick, rows_slow in ((1, slow_back_2), (2, slow_back_1)):
        state, part = pl.pallas_call(
            functools.partial(middle_kernel, freq_total, tick - 1, 3 - tick),
            out_shape=(state_shape, image_shape),
            in_specs=[SMEM] + [VMEM] * 7,
            out_specs=(VMEM, VMEM),
            scratch_shapes=held,
            cost_estimate=cost,
            name=f"tick{tick}",
        )(place, state, gathered, source, rows_slow, high, low, turn)
        images.append(move(part, tick - 3, f"image{tick}"))

    fields, image = pl.pallas_call(
        functools.partial(last_kernel, freq_total, ticks - 2, 0, sections - 1),
        out_shape=(shape(4, rows, points), image_shape),
        in_specs=[SMEM] + [VMEM] * 10,
        out_specs=(VMEM, VMEM),
        scratch_shapes=held,
        cost_estimate=cost,
        name="tick3",
    )(place, state, gathered, source, slow, high, low, turn, image_0, images[0], images[1])
    fields = move(fields, 1, "fields")
    own = lambda j: lax.dynamic_index_in_dim(image, (lane_pos + j) % lanes, 0, keepdims=True)
    total = own(0)
    for j in range(1, lanes):
        pairs = [(i, (i + j) % lanes) for i in range(lanes)]
        with jax.named_scope(f"lane{j}"):
            total = total + lax.ppermute(own(j), "lane", pairs)
    return fields[None], total


def solution(mesh):
    in_specs = (
        P("depth", None, "lane", None),
        P(None, "depth", None, "lane", None),
        P(None, None, "lane"),
        P("depth", None),
        P(),
    )
    out_specs = (P("depth", None, "lane", None), P(("depth", "lane"), None))
    body = functools.partial(per_device, mesh.shape["depth"], mesh.shape["lane"])
    return jax.shard_map(
        body, mesh=mesh, in_specs=in_specs, out_specs=out_specs, check_vma=False
    )
```

```python
import functools
import math

import jax
import jax.numpy as jnp
import numpy as np
from jax import lax
from jax.experimental import pallas as pl
from jax.experimental.pallas import tpu as pltpu
from jax.sharding import PartitionSpec as P


CODES = 16
OMEGA_LO = 0.25
OMEGA_STEP = 0.07
TWO_PI = 6.283185307179586
LANES = 128
OUTER = 8
F32 = jnp.float32
BF16 = jnp.bfloat16
VMEM = pl.BlockSpec(memory_space=pltpu.VMEM)
SMEM = pl.BlockSpec(memory_space=pltpu.SMEM)
SMALL = pltpu.CompilerParams(vmem_limit_bytes=8 * 1024 * 1024)


def dft_tables():
    j = np.arange(LANES)
    angle = 2.0 * np.pi * (np.outer(j, j) % LANES) / LANES
    c, s = np.cos(angle), np.sin(angle)
    full = np.block([[c, -s], [s, c]])
    high = np.asarray(full, dtype=BF16)
    low = np.asarray(full - high.astype(np.float64), dtype=BF16)
    k1 = np.repeat(np.arange(OUTER), 8)
    twist = 2.0 * np.pi * np.outer(k1, j) / (OUTER * LANES)
    turn = np.stack([np.cos(twist), np.sin(twist)]).astype(np.float32)
    return high, low, turn


def poly(coefs, x):
    out = jnp.full_like(x, coefs[-1])
    for c in reversed(coefs[:-1]):
        out = out * x + c
    return out


COS = [(-1.0) ** n / math.factorial(2 * n) for n in range(8)]
SIN = [(-1.0) ** n / math.factorial(2 * n + 1) for n in range(8)]


def cos_sin(x):
    sq = x * x
    return poly(COS, sq), x * poly(SIN, sq)


def code_turn(code):
    quarter = (code + 2) >> 2
    rest = (code - 4 * quarter).astype(F32) * (TWO_PI / CODES)
    c, s = cos_sin(rest)
    odd = (quarter & 1) == 1
    a = jnp.where(odd, -s, c)
    b = jnp.where(odd, c, s)
    flip = (quarter & 2) == 2
    return jnp.where(flip, -a, a), jnp.where(flip, -b, b)


def fourth(a, b, c, d, sign):
    s0 = (a[0] + c[0], a[1] + c[1])
    s1 = (a[0] - c[0], a[1] - c[1])
    s2 = (b[0] + d[0], b[1] + d[1])
    s3 = (b[0] - d[0], b[1] - d[1])
    plus = (s1[0] - s3[1], s1[1] + s3[0])
    minus = (s1[0] + s3[1], s1[1] - s3[0])
    x0 = (s0[0] + s2[0], s0[1] + s2[1])
    x2 = (s0[0] - s2[0], s0[1] - s2[1])
    return (x0, minus, x2, plus) if sign > 0 else (x0, plus, x2, minus)


def eighth(x, sign):
    even = fourth(x[0], x[2], x[4], x[6], sign)
    odd = fourth(x[1], x[3], x[5], x[7], sign)
    h = math.sqrt(0.5)
    o1, o2, o3 = odd[1], odd[2], odd[3]
    if sign > 0:
        w1 = ((o1[0] + o1[1]) * h, (o1[1] - o1[0]) * h)
        w2 = (o2[1], -o2[0])
        w3 = ((o3[1] - o3[0]) * h, -(o3[0] + o3[1]) * h)
    else:
        w1 = ((o1[0] - o1[1]) * h, (o1[1] + o1[0]) * h)
        w2 = (-o2[1], o2[0])
        w3 = (-(o3[0] + o3[1]) * h, (o3[0] - o3[1]) * h)
    w = (odd[0], w1, w2, w3)
    low = [(e[0] + v[0], e[1] + v[1]) for e, v in zip(even, w)]
    high = [(e[0] - v[0], e[1] - v[1]) for e, v in zip(even, w)]
    return low + high


def times(x, y):
    return (x[0] * y[0] - x[1] * y[1], x[0] * y[1] + x[1] * y[0])


def times_conj(x, y):
    return (x[0] * y[0] + x[1] * y[1], x[1] * y[0] - x[0] * y[1])


def mix(first, second, high_ref, low_ref):
    left = jnp.concatenate(first, axis=0)
    right = jnp.concatenate(second, axis=0)
    value = jnp.concatenate([left, right], axis=1)
    high = value.astype(BF16)
    low = (value - high.astype(F32)).astype(BF16)
    rows = value.shape[0]
    main = jnp.dot(
        jnp.concatenate([high, low], axis=0), high_ref[...], preferred_element_type=F32
    )
    rest = jnp.dot(high, low_ref[...], preferred_element_type=F32)
    out = main[:rows] + main[rows:] + rest
    split = lambda part: [part[8 * k : 8 * k + 8] for k in range(OUTER)]
    return split(out[:, :LANES]), split(out[:, LANES:])


def prepare(turn_ref):
    points = OUTER * LANES
    row = lax.broadcasted_iota(jnp.int32, (8, LANES), 0)
    column = lax.broadcasted_iota(jnp.int32, (8, LANES), 1)
    freq = lax.axis_index("lane") * 4 + (row & 3)
    omega = OMEGA_LO + OMEGA_STEP * freq.astype(F32)
    turn = [
        (turn_ref[0, 8 * k : 8 * k + 8, :], turn_ref[1, 8 * k : 8 * k + 8, :])
        for k in range(OUTER)
    ]
    kx_sq = []
    for k in range(OUTER):
        index = k + OUTER * column
        signed = jnp.where(index < points // 2, index, index - points)
        kx_sq.append((signed.astype(F32) * (TWO_PI / points)) ** 2)
    return omega, turn, kx_sq


def run_steps(tiles, setup, slow, high_ref, low_ref, image_ref, freq_total):
    points = OUTER * LANES
    omega, turn, kx_sq = setup
    mean = jnp.sum(slow, axis=1, keepdims=True) * (1.0 / points)
    for step in range(slow.shape[0]):
        ref = jnp.broadcast_to(mean[step : step + 1], (8, LANES))
        bound = (omega * ref) ** 2
        spec = eighth(tiles, 1)
        spec = [spec[0]] + [times_conj(spec[k], turn[k]) for k in range(1, OUTER)]
        re, im = mix([v[0] for v in spec], [v[1] for v in spec], high_ref, low_ref)
        moved = []
        for k in range(OUTER):
            kz_sq = bound - kx_sq[k]
            root = jnp.sqrt(jnp.abs(kz_sq))
            cos, sin = cos_sin(root)
            travels = kz_sq > 0.0
            scale = 1.0 / points
            prop = (
                jnp.where(travels, cos, jnp.exp(-root)) * scale,
                jnp.where(travels, sin, 0.0) * scale,
            )
            moved.append(times((re[k], im[k]), prop))
        im, re = mix([v[1] for v in moved], [v[0] for v in moved], high_ref, low_ref)
        back = [(re[0], im[0])] + [times((re[k], im[k]), turn[k]) for k in range(1, OUTER)]
        field = eighth(back, -1)
        tiles = []
        for a in range(OUTER):
            part = jnp.broadcast_to(
                slow[step : step + 1, LANES * a : LANES * (a + 1)], (8, LANES)
            )
            lens = cos_sin(omega * (part - ref))
            tiles.append(times(field[a], lens))
        for a in range(OUTER):
            re, im = tiles[a]
            both = re * pltpu.roll(re, 4, 0) - im * pltpu.roll(im, 4, 0)
            total = jnp.sum(both, axis=0, keepdims=True) * (0.5 / freq_total)
            image_ref[step : step + 1, LANES * a : LANES * (a + 1)] = total
    return tiles


def cut(a):
    return slice(LANES * a, LANES * (a + 1))


def natural_tiles(s_re, s_im, r_re, r_im):
    return [
        (
            jnp.concatenate([s_re[:, cut(a)], r_re[:, cut(a)]], axis=0),
            jnp.concatenate([s_im[:, cut(a)], -r_im[:, cut(a)]], axis=0),
        )
        for a in range(OUTER)
    ]


def state_tiles(state_ref):
    return [
        (state_ref[0, 8 * a : 8 * a + 8, :], state_ref[1, 8 * a : 8 * a + 8, :])
        for a in range(OUTER)
    ]


def put_state(state_ref, tiles):
    for a in range(OUTER):
        state_ref[0, 8 * a : 8 * a + 8, :] = tiles[a][0]
        state_ref[1, 8 * a : 8 * a + 8, :] = tiles[a][1]


def start_kernel(
    freq_total, table_ref, codes_ref, index_ref, shots_ref, fields_ref, high_ref, low_ref, turn_ref,
    own_ref, send_1_ref, send_2_ref, send_3_ref, slow_ref, state_ref, image_ref, source_ref,
    part_ref,
):
    place = lax.axis_index("depth")
    ticks, here = shots_ref.shape[0], shots_ref.shape[1]
    codes = codes_ref[...]
    column = lax.broadcasted_iota(jnp.int32, codes.shape, 1)
    turns = []
    for j in range(here):
        own = jnp.sum(
            jnp.where(column == place * here + j, codes, 0).astype(F32), axis=1, keepdims=True
        )
        turns.append(code_turn(own.astype(jnp.int32)))
    for t in range(ticks):
        re = im = 0.0
        for j in range(here):
            c = turns[j][0][4 * t : 4 * t + 4]
            s = turns[j][1][4 * t : 4 * t + 4]
            d_re, d_im = shots_ref[t, j, 0], shots_ref[t, j, 1]
            re = re + (c * d_re - s * d_im)
            im = im + (c * d_im + s * d_re)
        part_ref[t, 0] = re
        part_ref[t, 1] = im
    for j, ref in enumerate((own_ref, send_1_ref, send_2_ref, send_3_ref)):
        member = (place + j) & 3
        ref[...] = part_ref[jnp.where(member == 3, 3, 2 - member)]
    index = index_ref[...]
    slow = jnp.zeros(index.shape, F32)
    for level in range(table_ref.shape[0]):
        slow = jnp.where(index == level, table_ref[level], slow)
    slow_ref[...] = slow
    tiles = natural_tiles(fields_ref[0], fields_ref[1], fields_ref[2], fields_ref[3])
    setup = prepare(turn_ref)
    put_state(
        state_ref, run_steps(tiles, setup, slow, high_ref, low_ref, image_ref, freq_total)
    )
    shots = codes.shape[1]
    points = OUTER * LANES
    spacing = points // shots
    shot = lax.broadcasted_iota(jnp.int32, (shots, points), 0)
    cell = lax.broadcasted_iota(jnp.int32, (shots, points), 1)
    spread = jnp.where(cell == shot * spacing, 1.0, 0.0).astype(BF16)
    wide = jnp.dot(codes.astype(F32).astype(BF16), spread, preferred_element_type=F32)
    c, s = code_turn(wide.astype(jnp.int32))
    at_shot = lax.broadcasted_iota(jnp.int32, wide.shape, 1) % spacing == 0
    c = jnp.where(at_shot, c, 0.0)
    s = jnp.where(at_shot, s, 0.0)
    for t in range(ticks):
        source_ref[t, 0] = c[4 * t : 4 * t + 4]
        source_ref[t, 1] = s[4 * t : 4 * t + 4]


def pack_kernel(image_ref, image_1_ref, image_2_ref, own_ref, send_1_ref, send_2_ref, send_3_ref, sum_ref):
    lane = lax.axis_index("lane")
    sum_ref[...] = image_ref[...] + image_1_ref[...] + image_2_ref[...]
    for j, ref in enumerate((own_ref, send_1_ref, send_2_ref, send_3_ref)):
        ref[...] = sum_ref[pl.ds((lane + j) & 3, 1), :]


def finish_kernel(own_ref, a_ref, b_ref, c_ref, fields_in_ref, fields_ref, row_ref, sum_ref, sems):
    fields = pltpu.make_async_copy(fields_in_ref, fields_ref, sems.at[0])
    fields.start()
    sum_ref[...] = own_ref[...] + a_ref[...] + (b_ref[...] + c_ref[...])
    row = pltpu.make_async_copy(sum_ref, row_ref, sems.at[1])
    row.start()
    fields.wait()
    row.wait()


def later_kernel(
    freq_total, sections, state_in_ref, record_ref, source_ref, slow_a_ref, slow_b_ref, slow_c_ref,
    high_ref, low_ref, turn_ref, image_0_ref, field_ref, image_a_ref, image_b_ref, image_c_ref,
    held_ref, slow_ref, image_ref,
):
    place = lax.axis_index("depth")
    setup = prepare(turn_ref)
    held_ref[...] = state_in_ref[...]
    for i, ref in enumerate((slow_a_ref, slow_b_ref, slow_c_ref)):
        slow_ref[i] = ref[...]

    def tick(i, carry):
        @pl.when(place == 2 - i)
        def _():
            put_state(
                held_ref,
                natural_tiles(source_ref[i, 0], source_ref[i, 1], record_ref[0], record_ref[1]),
            )

        tiles = run_steps(
            state_tiles(held_ref), setup, slow_ref[i], high_ref, low_ref, image_ref.at[i], freq_total
        )
        put_state(held_ref, tiles)
        return carry

    lax.fori_loop(0, 3, tick, 0)
    image_a_ref[...] = image_ref[0]
    image_b_ref[...] = image_ref[1]
    image_c_ref[...] = image_ref[2] + image_0_ref[...]
    for a, (re, im) in enumerate(state_tiles(held_ref)):
        field_ref[0, :, cut(a)] = re[:4]
        field_ref[1, :, cut(a)] = im[:4]
        field_ref[2, :, cut(a)] = re[4:]
        field_ref[3, :, cut(a)] = -im[4:]

    @pl.when(place == sections - 1)
    def _():
        field_ref[0] = source_ref[3, 0]
        field_ref[1] = source_ref[3, 1]
        field_ref[2] = record_ref[0]
        field_ref[3] = record_ref[1]


def per_device(sections, lanes, fields_in, shot_data, codes, vel_index, slowness_table):
    return migrate(sections, lanes, fields_in, shot_data, codes, vel_index, slowness_table)


def migrate(sections, lanes, fields_in, shot_data, codes, vel_index, slowness_table):
    ticks, _, _, rows, points = shot_data.shape
    steps = vel_index.shape[0]
    freq_total = rows * lanes
    high, low, turn = dft_tables()
    turned = jnp.transpose(codes, (0, 2, 1)).reshape(ticks * rows, codes.shape[1])
    shape = lambda *s: jax.ShapeDtypeStruct(s, F32)
    state_shape = shape(2, OUTER * 8, LANES)
    image_shape = shape(steps, points)
    record_shape = shape(2, rows, points)
    row_shape = shape(1, points)

    def move(array, pairs, axis="depth"):
        return lax.ppermute(array, axis, pairs)

    def shift(array, by):
        return move(array, [(i, (i + by) % sections) for i in range(sections)])

    outs = pl.pallas_call(
        functools.partial(start_kernel, freq_total),
        out_shape=(record_shape,) * 4
        + (image_shape, state_shape, image_shape, shape(ticks, 2, rows, points)),
        in_specs=[SMEM] + [VMEM] * 7,
        out_specs=(VMEM,) * 8,
        scratch_shapes=[pltpu.VMEM((ticks, 2, rows, points), F32)],
        name="start",
    )(slowness_table, turned, vel_index, shot_data, fields_in[0], high, low, turn)
    record, sends = outs[0], outs[1:4]
    slow, state, image_0, source = outs[4:]

    def around(stride, size, by):
        return [
            (i, i + ((i // stride + by) % size - i // stride % size) * stride)
            for i in range(sections)
        ]

    arrived = [move(x, around(1, 4, j + 1)) for j, x in enumerate(sends)]
    slow_1 = shift(slow, 1)
    slow_2 = shift(slow, 2)
    state = shift(state, 3)
    record = record + arrived[0] + (arrived[1] + arrived[2])
    arrived = [move(record, around(8, 4, j)) for j in (1, 2, 3)]
    record = record + arrived[0] + (arrived[1] + arrived[2])
    far = lambda i, j: i ^ ((j & 1) * 4 + (j >> 1) * 32)
    arrived = [move(record, [(i, far(i, j)) for i in range(sections)]) for j in (1, 2, 3)]
    record = record + arrived[0] + (arrived[1] + arrived[2])

    fields, image_1, image_2, image = pl.pallas_call(
        functools.partial(later_kernel, freq_total, sections),
        out_shape=(shape(4, rows, points), image_shape, image_shape, image_shape),
        in_specs=[VMEM] * 10,
        out_specs=(VMEM,) * 4,
        scratch_shapes=[
            pltpu.VMEM((2, OUTER * 8, LANES), F32),
            pltpu.VMEM((3, steps, points), F32),
            pltpu.VMEM((3, steps, points), F32),
        ],
        compiler_params=SMALL,
        cost_estimate=pl.CostEstimate(
            flops=90_000_000, bytes_accessed=1_000_000, transcendentals=0
        ),
        name="later",
    )(state, record, source, slow_2, slow_1, slow, high, low, turn, image_0)
    image_1 = shift(image_1, -2)
    image_2 = shift(image_2, -1)
    fields = shift(fields, 1)
    rows_out = pl.pallas_call(
        pack_kernel,
        out_shape=(row_shape,) * 4,
        in_specs=[VMEM] * 3,
        out_specs=(VMEM,) * 4,
        scratch_shapes=[pltpu.VMEM((steps, points), F32)],
        compiler_params=SMALL,
        name="pack",
    )(image, image_1, image_2)
    arrived = []
    for j in (2, 1, 3):
        pairs = [(i, (i + j) % lanes) for i in range(lanes)]
        arrived.append(move(rows_out[j], pairs, "lane"))
    fields, total = pl.pallas_call(
        finish_kernel,
        out_shape=(shape(4, rows, points), row_shape),
        in_specs=[VMEM] * 5,
        out_specs=(pl.BlockSpec(memory_space=pl.ANY),) * 2,
        scratch_shapes=[pltpu.VMEM((1, points), F32), pltpu.SemaphoreType.DMA((2,))],
        compiler_params=SMALL,
        name="finish",
    )(rows_out[0], *arrived, fields)
    return fields[None], total


def solution(mesh):
    in_specs = (
        P("depth", None, "lane", None),
        P(None, "depth", None, "lane", None),
        P(None, None, "lane"),
        P("depth", None),
        P(),
    )
    out_specs = (P("depth", None, "lane", None), P(("depth", "lane"), None))
    body = functools.partial(per_device, mesh.shape["depth"], mesh.shape["lane"])
    return jax.shard_map(
        body, mesh=mesh, in_specs=in_specs, out_specs=out_specs, check_vma=False
    )
```

```python
import functools
import math

import jax
import jax.numpy as jnp
import numpy as np
from jax import lax
from jax.experimental import pallas as pl
from jax.experimental.pallas import tpu as pltpu
from jax.sharding import PartitionSpec as P


CODE_BITS = 4
POINT_BITS = 10
OMEGA_LO = 0.25
OMEGA_STEP = 0.07
TWO_PI = 6.283185307179586
LANES = 128
OUTER = 8
F32 = jnp.float32
BF16 = jnp.bfloat16
VMEM = pl.BlockSpec(memory_space=pltpu.VMEM)
SMEM = pl.BlockSpec(memory_space=pltpu.SMEM)
SMALL = pltpu.CompilerParams(vmem_limit_bytes=8 * 1024 * 1024)


def dft_tables():
    j = np.arange(LANES)
    angle = 2.0 * np.pi * (np.outer(j, j) % LANES) / LANES
    c, s = np.cos(angle), np.sin(angle)
    full = np.block([[c, -s], [s, c]])
    high = np.asarray(full, dtype=BF16)
    low = np.asarray(full - high.astype(np.float64), dtype=BF16)
    return high, low


def poly(coefs, x):
    out = jnp.full_like(x, coefs[-1])
    for c in reversed(coefs[:-1]):
        out = out * x + c
    return out


COS = [(-1.0) ** n / math.factorial(2 * n) for n in range(8)]
SIN = [(-1.0) ** n / math.factorial(2 * n + 1) for n in range(8)]


def cos_sin(x):
    sq = x * x
    return poly(COS, sq), x * poly(SIN, sq)


def whole_turn(index, bits):
    quarter = (index + (1 << (bits - 3))) >> (bits - 2)
    rest = (index - (quarter << (bits - 2))).astype(F32) * (TWO_PI / (1 << bits))
    c, s = cos_sin(rest)
    odd = (quarter & 1) == 1
    a = jnp.where(odd, -s, c)
    b = jnp.where(odd, c, s)
    flip = (quarter & 2) == 2
    return jnp.where(flip, -a, a), jnp.where(flip, -b, b)


def fourth(a, b, c, d, sign):
    s0 = (a[0] + c[0], a[1] + c[1])
    s1 = (a[0] - c[0], a[1] - c[1])
    s2 = (b[0] + d[0], b[1] + d[1])
    s3 = (b[0] - d[0], b[1] - d[1])
    plus = (s1[0] - s3[1], s1[1] + s3[0])
    minus = (s1[0] + s3[1], s1[1] - s3[0])
    x0 = (s0[0] + s2[0], s0[1] + s2[1])
    x2 = (s0[0] - s2[0], s0[1] - s2[1])
    return (x0, minus, x2, plus) if sign > 0 else (x0, plus, x2, minus)


def eighth(x, sign):
    even = fourth(x[0], x[2], x[4], x[6], sign)
    odd = fourth(x[1], x[3], x[5], x[7], sign)
    h = math.sqrt(0.5)
    o1, o2, o3 = odd[1], odd[2], odd[3]
    if sign > 0:
        w1 = ((o1[0] + o1[1]) * h, (o1[1] - o1[0]) * h)
        w2 = (o2[1], -o2[0])
        w3 = ((o3[1] - o3[0]) * h, -(o3[0] + o3[1]) * h)
    else:
        w1 = ((o1[0] - o1[1]) * h, (o1[1] + o1[0]) * h)
        w2 = (-o2[1], o2[0])
        w3 = (-(o3[0] + o3[1]) * h, (o3[0] - o3[1]) * h)
    w = (odd[0], w1, w2, w3)
    low = [(e[0] + v[0], e[1] + v[1]) for e, v in zip(even, w)]
    high = [(e[0] - v[0], e[1] - v[1]) for e, v in zip(even, w)]
    return low + high


def times(x, y):
    return (x[0] * y[0] - x[1] * y[1], x[0] * y[1] + x[1] * y[0])


def times_conj(x, y):
    return (x[0] * y[0] + x[1] * y[1], x[1] * y[0] - x[0] * y[1])


def mix(first, second, high_ref, low_ref):
    left = jnp.concatenate(first, axis=0)
    right = jnp.concatenate(second, axis=0)
    value = jnp.concatenate([left, right], axis=1)
    high = value.astype(BF16)
    low = (value - high.astype(F32)).astype(BF16)
    rows = value.shape[0]
    main = jnp.dot(
        jnp.concatenate([high, low], axis=0), high_ref[...], preferred_element_type=F32
    )
    rest = jnp.dot(high, low_ref[...], preferred_element_type=F32)
    out = main[:rows] + main[rows:] + rest
    split = lambda part: [part[8 * k : 8 * k + 8] for k in range(OUTER)]
    return split(out[:, :LANES]), split(out[:, LANES:])


def prepare():
    points = OUTER * LANES
    row = lax.broadcasted_iota(jnp.int32, (8, LANES), 0)
    column = lax.broadcasted_iota(jnp.int32, (8, LANES), 1)
    freq = lax.axis_index("lane") * 4 + (row & 3)
    omega = OMEGA_LO + OMEGA_STEP * freq.astype(F32)
    turn = [whole_turn(k * column, POINT_BITS) for k in range(OUTER)]
    kx_sq = []
    for k in range(OUTER):
        index = k + OUTER * column
        signed = jnp.where(index < points // 2, index, index - points)
        kx_sq.append((signed.astype(F32) * (TWO_PI / points)) ** 2)
    return omega, turn, kx_sq


def run_steps(tiles, setup, slow, high_ref, low_ref, image_ref, freq_total):
    points = OUTER * LANES
    omega, turn, kx_sq = setup
    mean = jnp.sum(slow, axis=1, keepdims=True) * (1.0 / points)
    for step in range(slow.shape[0]):
        ref = jnp.broadcast_to(mean[step : step + 1], (8, LANES))
        bound = (omega * ref) ** 2
        spec = eighth(tiles, 1)
        spec = [spec[0]] + [times_conj(spec[k], turn[k]) for k in range(1, OUTER)]
        re, im = mix([v[0] for v in spec], [v[1] for v in spec], high_ref, low_ref)
        moved = []
        for k in range(OUTER):
            kz_sq = bound - kx_sq[k]
            root = jnp.sqrt(jnp.abs(kz_sq))
            cos, sin = cos_sin(root)
            travels = kz_sq > 0.0
            scale = 1.0 / points
            prop = (
                jnp.where(travels, cos, jnp.exp(-root)) * scale,
                jnp.where(travels, sin, 0.0) * scale,
            )
            moved.append(times((re[k], im[k]), prop))
        im, re = mix([v[1] for v in moved], [v[0] for v in moved], high_ref, low_ref)
        back = [(re[0], im[0])] + [times((re[k], im[k]), turn[k]) for k in range(1, OUTER)]
        field = eighth(back, -1)
        tiles = []
        for a in range(OUTER):
            part = jnp.broadcast_to(
                slow[step : step + 1, LANES * a : LANES * (a + 1)], (8, LANES)
            )
            lens = cos_sin(omega * (part - ref))
            tiles.append(times(field[a], lens))
        for a in range(OUTER):
            re, im = tiles[a]
            both = re * pltpu.roll(re, 4, 0) - im * pltpu.roll(im, 4, 0)
            total = jnp.sum(both, axis=0, keepdims=True) * (0.5 / freq_total)
            image_ref[step : step + 1, LANES * a : LANES * (a + 1)] = total
    return tiles


def cut(a):
    return slice(LANES * a, LANES * (a + 1))


def natural_tiles(s_re, s_im, r_re, r_im):
    return [
        (
            jnp.concatenate([s_re[:, cut(a)], r_re[:, cut(a)]], axis=0),
            jnp.concatenate([s_im[:, cut(a)], -r_im[:, cut(a)]], axis=0),
        )
        for a in range(OUTER)
    ]


def state_tiles(state_ref):
    return [
        (state_ref[0, 8 * a : 8 * a + 8, :], state_ref[1, 8 * a : 8 * a + 8, :])
        for a in range(OUTER)
    ]


def put_state(state_ref, tiles):
    for a in range(OUTER):
        state_ref[0, 8 * a : 8 * a + 8, :] = tiles[a][0]
        state_ref[1, 8 * a : 8 * a + 8, :] = tiles[a][1]


def start_kernel(
    table_hbm, codes_hbm, index_hbm, shots_hbm, own_ref, send_1_ref, send_2_ref, send_3_ref,
    slow_ref, part_ref, table_ref, codes_ref, index_ref, shots_ref, sems,
):
    copies = [
        pltpu.make_async_copy(a, b, sems.at[i])
        for i, (a, b) in enumerate(
            (
                (table_hbm, table_ref),
                (codes_hbm, codes_ref),
                (index_hbm, index_ref),
                (shots_hbm, shots_ref),
            )
        )
    ]
    for copy in copies:
        copy.start()
    for copy in copies:
        copy.wait()
    place = lax.axis_index("depth")
    ticks, here = shots_ref.shape[0], shots_ref.shape[1]
    codes = codes_ref[...]
    column = lax.broadcasted_iota(jnp.int32, codes.shape, 1)
    turns = []
    for j in range(here):
        own = jnp.sum(
            jnp.where(column == place * here + j, codes, 0).astype(F32), axis=1, keepdims=True
        )
        turns.append(whole_turn(own.astype(jnp.int32), CODE_BITS))
    for t in range(ticks):
        re = im = 0.0
        for j in range(here):
            c = turns[j][0][4 * t : 4 * t + 4]
            s = turns[j][1][4 * t : 4 * t + 4]
            d_re, d_im = shots_ref[t, j, 0], shots_ref[t, j, 1]
            re = re + (c * d_re - s * d_im)
            im = im + (c * d_im + s * d_re)
        part_ref[t, 0] = re
        part_ref[t, 1] = im
    for j, ref in enumerate((own_ref, send_1_ref, send_2_ref, send_3_ref)):
        member = (place & 3) ^ j
        ref[...] = part_ref[jnp.where(member == 3, 3, 2 - member)]
    index = index_ref[...]
    slow = jnp.zeros(index.shape, F32)
    for level in range(table_ref.shape[0]):
        slow = jnp.where(index == level, table_ref[level], slow)
    slow_ref[...] = slow


def first_kernel(
    freq_total, codes_ref, slow_in_ref, fields_ref, high_ref, low_ref, state_ref, image_ref,
    source_ref,
):
    codes = codes_ref[...]
    ticks = codes.shape[0] // 4
    slow = slow_in_ref[...]
    tiles = natural_tiles(fields_ref[0], fields_ref[1], fields_ref[2], fields_ref[3])
    setup = prepare()
    put_state(
        state_ref, run_steps(tiles, setup, slow, high_ref, low_ref, image_ref, freq_total)
    )
    shots = codes.shape[1]
    points = OUTER * LANES
    spacing = points // shots
    shot = lax.broadcasted_iota(jnp.int32, (shots, points), 0)
    cell = lax.broadcasted_iota(jnp.int32, (shots, points), 1)
    spread = jnp.where(cell == shot * spacing, 1.0, 0.0).astype(BF16)
    wide = jnp.dot(codes.astype(F32).astype(BF16), spread, preferred_element_type=F32)
    c, s = whole_turn(wide.astype(jnp.int32), CODE_BITS)
    at_shot = lax.broadcasted_iota(jnp.int32, wide.shape, 1) % spacing == 0
    c = jnp.where(at_shot, c, 0.0)
    s = jnp.where(at_shot, s, 0.0)
    for t in range(ticks):
        source_ref[t, 0] = c[4 * t : 4 * t + 4]
        source_ref[t, 1] = s[4 * t : 4 * t + 4]


def pack_kernel(image_ref, image_1_ref, image_2_ref, own_ref, send_1_ref, send_2_ref, send_3_ref, sum_ref):
    lane = lax.axis_index("lane")
    sum_ref[...] = image_ref[...] + image_1_ref[...] + image_2_ref[...]
    for j, ref in enumerate((own_ref, send_1_ref, send_2_ref, send_3_ref)):
        ref[...] = sum_ref[pl.ds(lane ^ j, 1), :]


def finish_kernel(own_ref, a_ref, b_ref, c_ref, fields_in_ref, fields_ref, row_ref, sum_ref, sems):
    fields = pltpu.make_async_copy(fields_in_ref, fields_ref, sems.at[0])
    fields.start()
    sum_ref[...] = own_ref[...] + a_ref[...] + (b_ref[...] + c_ref[...])
    row = pltpu.make_async_copy(sum_ref, row_ref, sems.at[1])
    row.start()
    fields.wait()
    row.wait()


def later_kernel(
    freq_total, sections, tick, last, state_in_ref, record_ref, source_ref, slow_ref, high_ref,
    low_ref, *rest,
):
    if last:
        image_0_ref, out_ref, image_ref, held_ref = rest
    else:
        out_ref, image_ref, held_ref = rest
    place = lax.axis_index("depth")
    inject = place == 2 - tick

    @pl.when(inject)
    def _():
        put_state(
            held_ref,
            natural_tiles(source_ref[tick, 0], source_ref[tick, 1], record_ref[0], record_ref[1]),
        )

    @pl.when(jnp.logical_not(inject))
    def _():
        held_ref[...] = state_in_ref[...]

    tiles = run_steps(
        state_tiles(held_ref), prepare(), slow_ref[...], high_ref, low_ref, image_ref, freq_total
    )
    if not last:
        put_state(out_ref, tiles)
        return
    image_ref[...] += image_0_ref[...]
    for a, (re, im) in enumerate(tiles):
        out_ref[0, :, cut(a)] = re[:4]
        out_ref[1, :, cut(a)] = im[:4]
        out_ref[2, :, cut(a)] = re[4:]
        out_ref[3, :, cut(a)] = -im[4:]

    @pl.when(place == sections - 1)
    def _():
        out_ref[0] = source_ref[tick + 1, 0]
        out_ref[1] = source_ref[tick + 1, 1]
        out_ref[2] = record_ref[0]
        out_ref[3] = record_ref[1]


def per_device(sections, lanes, fields_in, shot_data, codes, vel_index, slowness_table):
    return migrate(sections, lanes, fields_in, shot_data, codes, vel_index, slowness_table)


def migrate(sections, lanes, fields_in, shot_data, codes, vel_index, slowness_table):
    ticks, _, _, rows, points = shot_data.shape
    steps = vel_index.shape[0]
    freq_total = rows * lanes
    high, low = dft_tables()
    turned = jnp.transpose(codes, (0, 2, 1)).reshape(ticks * rows, codes.shape[1])
    shape = lambda *s: jax.ShapeDtypeStruct(s, F32)
    state_shape = shape(2, OUTER * 8, LANES)
    image_shape = shape(steps, points)
    record_shape = shape(2, rows, points)
    row_shape = shape(1, points)

    def move(array, pairs, axis="depth"):
        return lax.ppermute(array, axis, pairs)

    def shift(array, by):
        return move(array, [(i, (i + by) % sections) for i in range(sections)])

    given = (slowness_table, turned, vel_index, shot_data)
    outs = pl.pallas_call(
        start_kernel,
        out_shape=(record_shape,) * 4 + (image_shape,),
        in_specs=[pl.BlockSpec(memory_space=pltpu.HBM)] * 4,
        out_specs=(VMEM,) * 5,
        scratch_shapes=[
            pltpu.VMEM((ticks, 2, rows, points), F32),
            pltpu.SMEM(slowness_table.shape, F32),
            pltpu.VMEM(turned.shape, jnp.int32),
            pltpu.VMEM(vel_index.shape, jnp.int32),
            pltpu.VMEM(shot_data.shape, F32),
            pltpu.SemaphoreType.DMA((4,)),
        ],
        compiler_params=SMALL,
        name="start",
    )(*(pltpu.with_memory_space_constraint(x, pltpu.HBM) for x in given))
    record, sends, slow = outs[0], outs[1:4], outs[4]
    state, image_0, source = pl.pallas_call(
        functools.partial(first_kernel, freq_total),
        out_shape=(state_shape, image_shape, shape(ticks, 2, rows, points)),
        in_specs=[VMEM] * 5,
        out_specs=(VMEM,) * 3,
        compiler_params=SMALL,
        cost_estimate=pl.CostEstimate(
            flops=30_000_000, bytes_accessed=1_000_000, transcendentals=0
        ),
        name="tick0",
    )(turned, slow, fields_in[0], high, low)

    def swap(array, by):
        return move(array, [(i, i ^ by) for i in range(sections)])

    arrived = [swap(x, j + 1) for j, x in enumerate(sends)]
    slow_1 = shift(slow, 1)
    slow_2 = shift(slow, 2)
    state = shift(state, 3)
    record = record + arrived[0] + (arrived[1] + arrived[2])
    arrived = [swap(record, 8 * j) for j in (1, 2, 3)]
    record = record + arrived[0] + (arrived[1] + arrived[2])
    arrived = [swap(record, (j & 1) * 4 + (j >> 1) * 32) for j in (1, 2, 3)]
    record = record + arrived[0] + (arrived[1] + arrived[2])

    def later(tick, state, slow_rows, image_0=()):
        last = tick == 2
        return pl.pallas_call(
            functools.partial(later_kernel, freq_total, sections, tick, last),
            out_shape=(shape(4, rows, points) if last else state_shape, image_shape),
            in_specs=[VMEM] * (6 + len(image_0)),
            out_specs=(VMEM,) * 2,
            scratch_shapes=[pltpu.VMEM((2, OUTER * 8, LANES), F32)],
            compiler_params=SMALL,
            cost_estimate=pl.CostEstimate(
                flops=30_000_000, bytes_accessed=1_000_000, transcendentals=0
            ),
        )(state, record, source, slow_rows, high, low, *image_0)

    state, image_1 = later(0, state, slow_2)
    image_1 = shift(image_1, -2)
    state, image_2 = later(1, state, slow_1)
    image_2 = shift(image_2, -1)
    fields, image = later(2, state, slow, (image_0,))
    fields = shift(fields, 1)
    rows_out = pl.pallas_call(
        pack_kernel,
        out_shape=(row_shape,) * 4,
        in_specs=[VMEM] * 3,
        out_specs=(VMEM,) * 4,
        scratch_shapes=[pltpu.VMEM((steps, points), F32)],
        compiler_params=SMALL,
        name="pack",
    )(image, image_1, image_2)
    arrived = []
    for j in (2, 1, 3):
        pairs = [(i, i ^ j) for i in range(lanes)]
        arrived.append(move(rows_out[j], pairs, "lane"))
    fields, total = pl.pallas_call(
        finish_kernel,
        out_shape=(shape(4, rows, points), row_shape),
        in_specs=[VMEM] * 5,
        out_specs=(pl.BlockSpec(memory_space=pl.ANY),) * 2,
        scratch_shapes=[pltpu.VMEM((1, points), F32), pltpu.SemaphoreType.DMA((2,))],
        compiler_params=SMALL,
        name="finish",
    )(rows_out[0], *arrived, fields)
    return fields[None], total


def solution(mesh):
    in_specs = (
        P("depth", None, "lane", None),
        P(None, "depth", None, "lane", None),
        P(None, None, "lane"),
        P("depth", None),
        P(),
    )
    out_specs = (P("depth", None, "lane", None), P(("depth", "lane"), None))
    body = functools.partial(per_device, mesh.shape["depth"], mesh.shape["lane"])
    return jax.shard_map(
        body, mesh=mesh, in_specs=in_specs, out_specs=out_specs, check_vma=False
    )
```
